32 devices in a mesh: shift: 2 (over y), expert: 4 (over z), shard: 4 (over x, core).
Axes of the slice: x: 2, y: 2, z: 4, core: 2. Of those that a mesh axis runs over, the one named last changes fastest.
Arguments:
- master_gate: float32 [128, 2048, 1024], P(('shift', 'expert'), 'shard'), parts along dimension 0, may hold values from -0.1875 to 0.1875
- master_up: float32 [128, 2048, 1024], P(('shift', 'expert'), 'shard'), parts along dimension 0, may hold values from -0.1875 to 0.1875
- router_weight: float32 [4096, 64], P(('shift', 'shard'), 'expert'), parts along dimension 0, may hold values from -0.125 to 0.125
- router_gain: float32 [4096], P(('shift', 'shard')), parts along dimension 0, may hold values from 0.25 to 1.75
Outputs:
- final_gate: bfloat16 [128, 2048, 1024], P(('shift', 'expert'), None, 'shard'), parts along dimension 0
- final_up: bfloat16 [128, 2048, 1024], P(('shift', 'expert'), None, 'shard'), parts along dimension 0
- scale_gate: float32 [128, 1024], P(('shift', 'expert'), 'shard'), parts along dimension 0
- scale_up: float32 [128, 1024], P(('shift', 'expert'), 'shard'), parts along dimension 0
- serve_router: bfloat16 [4096, 64], P('shift'), parts along dimension 0
The draws below stay inside these ranges and needn't reach their ends.
There are 2 independent parts, one for each index of `shift`. The reference program is written for one: setup_inputs(seed, part) draws one part's arguments, and reference() takes and returns one part's arrays. A program takes and returns all parts, laid end to end along the dimension named above; each array names one. Nothing has to cross between parts.
All inputs are finite; a program needn't handle non-finite values. Where the reference program divides by a largest or mean magnitude, that divisor is 1e-20 or more.
Results may differ from the reference program's by a relative error of at most 0.001.
Values may be sent and summed in bfloat16 or wider, within the bound.
A program may use at most 256 MiB of HBM per device.

```python
import jax
import jax.numpy as jnp

EXPERTS = 64
D_MODEL = 2048
D_EXPERT = 1024


def spiked(values, rng, source, target, blocks, factor):
    def block_of(axis_at):
        return (jnp.arange(values.shape[axis_at]) // (values.shape[axis_at] // blocks)).reshape((-1,) + (1,) * (values.ndim - 1 - axis_at))

    first = jax.random.permutation(rng, blocks)[block_of(target)]
    second = (block_of(target) + blocks // 2) % blocks
    return jnp.where((block_of(source) == first) | (block_of(source) == second), factor * values, values)


def block_levels(stream_key, shape, split, smallest, high):
    gain = 1.0
    for dim, shards_of in split:
        steps = jax.random.uniform(jax.random.fold_in(jax.random.fold_in(stream_key, 6), dim), (shards_of,), jnp.float32, smallest / len(split), high / len(split))
        gain = gain * jnp.repeat(jnp.exp(steps), shape[dim] // shards_of).reshape((-1,) + (1,) * (len(shape) - 1 - dim))
    return gain


def bell_draw(rng, shape, width, reach, cuts=(), held_as=jnp.bfloat16):
    values = jax.random.normal(rng, shape, jnp.float32) * width
    if len(cuts) > 0:
        values = block_levels(rng, shape, cuts, -0.22, 0.18) * values
    return jnp.clip(values, min=-reach, max=reach).astype(held_as)


def bell_draw_with(stream_key, dims, spread, most, pieces, heavy, kind=jnp.bfloat16):
    array = spread * jax.random.normal(stream_key, dims, jnp.float32)
    if pieces:
        array = array * block_levels(stream_key, dims, pieces, -0.22, 0.18)
    return jnp.clip(spiked(array, jax.random.fold_in(stream_key, 3), *heavy), -most, most).astype(kind)


def setup_inputs(seed: int = 0, part: int = 0) -> dict:
    seeds = jax.random.split(jax.random.key(seed), 5)
    part_splits = jax.random.split(jax.random.fold_in(seeds[4], part), 5)
    master_gate = bell_draw_with(part_splits[0], (EXPERTS, D_MODEL, D_EXPERT), D_MODEL ** -0.5, 0.1875, ((0, 4), (1, 4)), (1, 2, 4, 2.0), jnp.float32)
    master_up = bell_draw_with(part_splits[1], (EXPERTS, D_MODEL, D_EXPERT), D_MODEL ** -0.5, 0.1875, ((0, 4), (1, 4)), (1, 2, 4, 2.0), jnp.float32)
    router_weight = bell_draw(part_splits[2], (D_MODEL, EXPERTS), D_MODEL ** -0.5, 0.125, ((0, 4), (1, 4)), jnp.float32)
    router_gain = jnp.clip(1.0 + 0.15 * jax.random.normal(part_splits[3], (D_MODEL,), jnp.float32), 0.25, 1.75)
    return dict(master_gate=master_gate, master_up=master_up, router_weight=router_weight, router_gain=router_gain)


def reference(master_gate, master_up, router_weight, router_gain):
    scale_gate = jnp.max(jnp.abs(master_gate), axis=1)
    final_gate = (master_gate / jnp.expand_dims(scale_gate, 1)).astype(jnp.bfloat16)
    scale_up = jnp.max(jnp.abs(master_up), axis=1)
    final_up = (master_up / jnp.expand_dims(scale_up, 1)).astype(jnp.bfloat16)
    serve_router = (router_weight * router_gain[:, None]).astype(jnp.bfloat16)
    return final_gate, final_up, scale_gate, scale_up, serve_router
```

```python
import functools

import jax
import jax.numpy as jnp
from jax import lax
from jax.experimental import pallas as pl
from jax.experimental.pallas import tpu as pltpu
from jax.sharding import PartitionSpec as P

MESH = pl.DeviceIdType.MESH
LANES = 128
LAG = 6
AHEAD = 2
SLOTS = 5


def exchange(
    n, groups, gate, up, router, narrow, tail, scales, routers, held, out, mine, theirs,
    load_sem, max_send, max_recv, send_sem, recv_sem, keep_sem, rt_send, rt_recv, rt_keep,
):
    me, group = lax.axis_index("shard"), lax.axis_index("expert")
    items, rows, width, depth = 2 * gate.shape[0], gate.shape[1], out.shape[3], held.shape[0]
    blocks, per = gate.shape[2] // LANES, width // LANES
    others = [(j, g) for g in range(groups) for j in range(n) if (j, g) != (0, 0)]

    def peer(j):
        return lax.rem(me + j, n)

    def device(j, g):
        return {"shard": peer(j), "expert": lax.rem(group + g, groups)}

    def load(k):
        slot, expert = lax.rem(k, depth), k // 2

        @pl.when(lax.rem(k, 2) == 0)
        def _():
            pltpu.make_async_copy(gate.at[expert], held.at[slot], load_sem.at[slot]).start()

        @pl.when(lax.rem(k, 2) == 1)
        def _():
            pltpu.make_async_copy(up.at[expert], held.at[slot], load_sem.at[slot]).start()

    def send_max(k, j):
        return pltpu.make_async_remote_copy(
            mine.at[k], theirs.at[k, j - 1], max_send, max_recv.at[k],
            device_id=device(j, 0), device_id_type=MESH,
        )

    def place(k):
        return narrow.at[lax.rem(k, 2), k // 2, pl.ds(pl.multiple_of(me * rows, rows), rows)]

    def send(k, j):
        slot = lax.rem(k, SLOTS)
        return pltpu.make_async_remote_copy(
            out.at[slot, peer(j)], place(k), send_sem.at[slot], recv_sem.at[j - 1],
            device_id=device(j, 0), device_id_type=MESH,
        )

    def keep(k):
        slot = lax.rem(k, SLOTS)
        return pltpu.make_async_copy(out.at[slot, me], place(k), keep_sem.at[slot])

    def leave(k):
        slot = lax.rem(k, SLOTS)
        return pltpu.make_async_copy(out.at[slot], tail.at[:, lax.rem(k, 2)], keep_sem.at[slot])

    def sent(k):
        slot = lax.rem(k, SLOTS)
        ref = out.at[slot, pl.ds(0, n - 1)]
        pltpu.make_async_copy(ref, ref, send_sem.at[slot]).wait()
        keep(k).wait()

    for k in range(AHEAD):
        load(jnp.int32(k))
    barrier = pltpu.get_barrier_semaphore()
    for j, g in others:
        pl.semaphore_signal(barrier, inc=1, device_id=device(j, g), device_id_type=MESH)
    pl.semaphore_wait(barrier, len(others))

    home = routers.at[group * n + me]
    for j, g in others:
        pltpu.make_async_remote_copy(
            router, home, rt_send, rt_recv, device_id=device(j, g), device_id_type=MESH
        ).start()
    own = pltpu.make_async_copy(router, home, rt_keep)
    own.start()

    def step(k, _):
        @pl.when(k + AHEAD < items)
        def _():
            load(k + AHEAD)

        @pl.when(k < items)
        def _():
            slot = lax.rem(k, depth)
            pltpu.make_async_copy(gate.at[0], held.at[slot], load_sem.at[slot]).wait()
            for b in range(blocks):
                column = held[slot, :, b * LANES : (b + 1) * LANES]
                mine[k, b : b + 1, :] = jnp.max(jnp.abs(column), axis=0, keepdims=True)
            for j in range(1, n):
                send_max(k, j).start()

        q = k - LAG

        @pl.when(q >= 0)
        def _():
            @pl.when(q >= SLOTS)
            def _():
                sent(q - SLOTS)

            pltpu.make_async_copy(theirs.at[q], theirs.at[q], max_recv.at[q]).wait()
            scale = mine[q]
            for j in range(1, n):
                scale = jnp.maximum(scale, theirs[q, j - 1])
            scales[q] = scale
            slot, source = lax.rem(q, SLOTS), lax.rem(q, depth)
            for b in range(blocks):
                at = (b % per) * LANES
                column = held[source, :, b * LANES : (b + 1) * LANES]
                out[slot, b // per, :, at : at + LANES] = (column / scale[b : b + 1]).astype(
                    jnp.bfloat16
                )

            @pl.when(q < items - 2)
            def _():
                for j in range(1, n):
                    send(q, j).start()
                keep(q).start()

            @pl.when(q >= items - 2)
            def _():
                leave(q).start()

        return 0

    lax.fori_loop(0, items + LAG, step, 0)

    def drain(k, _):
        sent(k)
        return 0

    lax.fori_loop(items - SLOTS, items - 2, drain, 0)
    for k in (items - 2, items - 1):
        leave(jnp.int32(k)).wait()
    pltpu.make_async_copy(theirs, theirs, max_send).wait()
    for j in range(1, n):
        ref = narrow.at[:, :, pl.ds(pl.multiple_of(peer(n - j) * rows, rows), rows)]
        pltpu.make_async_copy(ref, ref, recv_sem.at[j - 1]).wait()
    rest = routers.at[pl.ds(0, n * groups - 1)]
    pltpu.make_async_copy(rest, rest, rt_send).wait()
    pltpu.make_async_copy(rest, rest, rt_recv).wait()
    own.wait()


def spread(narrow, gate, up):
    gate[...] = narrow[0]
    up[...] = narrow[1]


def finish(arrived, gate_in, up_in, gate, up):
    gate[...] = arrived[:, 0]
    up[...] = arrived[:, 1]


def by_kernel(n, groups, gate, up, router, gain):
    experts, rows, columns = gate.shape
    width, items, depth = columns // n, 2 * experts, LAG + AHEAD + 1
    tokens, share = router.shape
    part = (router * gain[:, None]).astype(jnp.bfloat16).reshape(-1, LANES)
    anywhere = pl.BlockSpec(memory_space=pl.ANY)
    inside = pl.BlockSpec(memory_space=pltpu.VMEM)
    dma = pltpu.SemaphoreType.DMA
    narrow, tail, scales, routers = pl.pallas_call(
        functools.partial(exchange, n, groups),
        name="exchange",
        out_shape=(
            jax.ShapeDtypeStruct((2, experts - 1, n * rows, width), jnp.bfloat16),
            jax.ShapeDtypeStruct((n, 2, rows, width), jnp.bfloat16),
            jax.ShapeDtypeStruct((items, columns // LANES, LANES), jnp.float32),
            jax.ShapeDtypeStruct((groups * n,) + part.shape, jnp.bfloat16),
        ),
        in_specs=[anywhere, anywhere, inside],
        out_specs=(anywhere, anywhere, inside, anywhere),
        scratch_shapes=[
            pltpu.VMEM((depth, rows, columns), jnp.float32),
            pltpu.VMEM((SLOTS, n, rows, width), jnp.bfloat16),
            pltpu.VMEM((items, columns // LANES, LANES), jnp.float32),
            pltpu.VMEM((items, n - 1, columns // LANES, LANES), jnp.float32),
            dma((depth,)),
            dma,
            dma((items,)),
            dma((SLOTS,)),
            dma((n - 1,)),
            dma((SLOTS,)),
            dma,
            dma,
            dma,
        ],
        compiler_params=pltpu.CompilerParams(collective_id=0, has_side_effects=True),
    )(gate, up, part)
    arrived = lax.all_to_all(tail, "shard", split_axis=0, concat_axis=0, tiled=True)
    finals = (jax.ShapeDtypeStruct((experts, n * rows, width), jnp.bfloat16),) * 2
    most = pl.pallas_call(
        spread,
        name="spread",
        grid=(experts - 1,),
        out_shape=finals,
        in_specs=[pl.BlockSpec((2, 1, n * rows, width), lambda e: (0, e, 0, 0))],
        out_specs=(pl.BlockSpec((1, n * rows, width), lambda e: (e, 0, 0)),) * 2,
        cost_estimate=pl.CostEstimate(flops=0, bytes_accessed=4 * narrow.size, transcendentals=0),
    )(narrow)
    final_gate, final_up = pl.pallas_call(
        finish,
        name="finish",
        grid=(n,),
        out_shape=finals,
        in_specs=[
            pl.BlockSpec((1, 2, rows, width), lambda s: (s, 0, 0, 0)), anywhere, anywhere,
        ],
        out_specs=(pl.BlockSpec((1, rows, width), lambda s: (experts - 1, s, 0)),) * 2,
        input_output_aliases={1: 0, 2: 1},
    )(arrived, *most)
    scales = lax.dynamic_slice_in_dim(
        scales.reshape(experts, 2, columns), lax.axis_index("shard") * width, width, axis=2
    )
    serve_router = routers.reshape(groups, n * tokens, share).transpose(1, 0, 2)
    return (
        final_gate, final_up, scales[:, 0], scales[:, 1],
        serve_router.reshape(n * tokens, groups * share),
    )


def by_collectives(gate, up, router, gain):
    scale_gate, scale_up = lax.pmax(
        (jnp.max(jnp.abs(gate), axis=1), jnp.max(jnp.abs(up), axis=1)), "shard"
    )

    def serve(master, scale):
        narrow = (master / jnp.expand_dims(scale, 1)).astype(jnp.bfloat16)
        final = lax.all_to_all(narrow, "shard", split_axis=2, concat_axis=1, tiled=True)
        width = final.shape[2]
        return final, lax.dynamic_slice_in_dim(
            scale, lax.axis_index("shard") * width, width, axis=1
        )

    final_gate, scale_gate = serve(gate, scale_gate)
    final_up, scale_up = serve(up, scale_up)
    part = (router * gain[:, None]).astype(jnp.bfloat16)
    rows = lax.all_gather(part, "shard", axis=0, tiled=True)
    return final_gate, final_up, scale_gate, scale_up, lax.all_gather(rows, "expert", axis=1, tiled=True)


def solution(mesh):
    n, groups = mesh.shape["shard"], mesh.shape["expert"]

    def shards(gate, up, router, gain):
        aligned = gate.shape[2] % (n * LANES) == 0 and gate.shape[1] % 16 == 0
        aligned = aligned and 2 * gate.shape[0] > SLOTS
        if n > 1 and aligned and router.size % (16 * LANES) == 0:
            return by_kernel(n, groups, gate, up, router, gain)
        return by_collectives(gate, up, router, gain)

    return jax.shard_map(
        shards,
        mesh=mesh,
        in_specs=(
            P(("shift", "expert"), "shard", None),
            P(("shift", "expert"), "shard", None),
            P(("shift", "shard"), "expert"),
            P(("shift", "shard")),
        ),
        out_specs=(
            P(("shift", "expert"), None, "shard"),
            P(("shift", "expert"), None, "shard"),
            P(("shift", "expert"), "shard"),
            P(("shift", "expert"), "shard"),
            P("shift", None),
        ),
        check_vma=False,
    )
```
